32 devices in a mesh: row: 8 (over z, x), col: 4 (over y, core).
Axes of the slice: x: 2, y: 2, z: 4, core: 2. Of those that a mesh axis runs over, the one named last changes fastest.
Arguments:
- hidden_in: bfloat16 [32, 512, 1024], P('row', 'col'), may hold values from -6 to 6
- first_values: bfloat16 [32, 1024, 512], P('row', 'col'), may hold values from -6 to 6
- lengths: int32 [32, 4], P('row'), may hold values from 1 to 256, 512 in all within a row
- places: int32 [32, 512], P('row'), may hold values from 0 to 511, each once within a row
- gain_attn: float32 [1024], replicated, may hold values from 0.1 to 1.9
- gain_ffn: float32 [1024], replicated, may hold values from 0.1 to 1.9
- w_query: bfloat16 [1024, 1024], P('row', 'col'), may hold values from -0.1875 to 0.1875
- w_key: bfloat16 [1024, 1024], P('row', 'col'), may hold values from -0.1875 to 0.1875
- w_value: bfloat16 [1024, 1024], P('row', 'col'), may hold values from -0.1875 to 0.1875
- w_out: bfloat16 [1024, 1024], P('col', 'row'), may hold values from -3 to 3
- w_gate: bfloat16 [1024, 2816], P('row', 'col'), may hold values from -0.1875 to 0.1875
- w_up: bfloat16 [1024, 2816], P('row', 'col'), may hold values from -0.1875 to 0.1875
- w_down: bfloat16 [2816, 1024], P('col', 'row'), may hold values from -0.109375 to 0.109375
- out_grad: bfloat16 [32, 512, 1024], P('row', 'col'), may hold values from -6 to 6
Outputs:
- layer_out: bfloat16 [32, 512, 1024], P('row', 'col')
- grad_hidden: float32 [32, 512, 1024], P('row', 'col')
- grad_first_values: float32 [32, 1024, 512], P('row', 'col')
- grad_gain_attn: float32 [1024], replicated
- grad_gain_ffn: float32 [1024], replicated
- grad_w_query: float32 [1024, 1024], P('row', 'col')
- grad_w_key: float32 [1024, 1024], P('row', 'col')
- grad_w_value: float32 [1024, 1024], P('row', 'col')
- grad_w_out: float32 [1024, 1024], P('col', 'row')
- grad_w_gate: float32 [1024, 2816], P('row', 'col')
- grad_w_up: float32 [1024, 2816], P('row', 'col')
- grad_w_down: float32 [2816, 1024], P('col', 'row')
The draws below stay inside these ranges and needn't reach their ends.
Inputs may be any that keep to these rules, and one draw needn't show every extreme that they name: Each row of lengths sums to 512; the largest length in the draw is 256. Each row of places holds every number of 0 to 511 once.
All inputs are finite; a program needn't handle non-finite values.
Results may differ from the reference program's by a relative error of at most 0.015.
Values may be sent and summed in bfloat16 or wider, within the bound.
A program may use at most 192 MiB of HBM per device.

```python
import math
import jax
import jax.numpy as jnp
import numpy as np
from jax import lax

D = 1024
HEADS = 16
HEAD_DIM = 64
FF = 2816
TOK_MB = 512
NSEQ = 4
LMAX = 256
SLOTS = 32


def steps_of(own_key, extent, split, least, high):
    level, own = 1.0, jax.random.fold_in(own_key, 6)
    for dim, blocks in split:
        draws = jnp.exp(jax.random.uniform(jax.random.fold_in(own, dim), (blocks,), jnp.float32, least / len(split), high / len(split)))
        level = level * jnp.repeat(draws, extent[dim] // blocks).reshape([-1 if axis == dim else 1 for axis in range(len(extent))])
    return level


def length_profile(amount, total, bound, slope):
    weights = [(1 << 20) // math.isqrt(rank ** slope) + 1 for rank in range(2, amount + 1)]
    surplus, given = total - bound - (amount - 1), [1] * (amount - 1)
    while surplus > 0:
        movable = [i for i in range(amount - 1) if given[i] < bound]
        whole, left = sum([weights[i] for i in movable]), surplus
        for i in movable:
            extra = min(bound - given[i], max(1, left * weights[i] // whole), surplus)
            given[i] = given[i] + extra
            surplus = surplus - extra
    return np.array([bound] + given)


def ragged(own_key, amount, total, most, slope):
    if amount == 2:
        one = jax.random.randint(own_key, (), max(1, total - most), min(most, total - 1) + 1)
        return jnp.stack([one, total - one])
    sizes = jnp.asarray(length_profile(amount, total, most, slope), jnp.int32)
    couples = (amount - 1) // 2
    donor, sink = sizes[1:1 + 2 * couples:2], sizes[2:2 + 2 * couples:2]
    room = jnp.minimum(donor - 1, most - sink)
    moved = jax.random.randint(jax.random.fold_in(own_key, 1), (couples,), 0, 1 << 20) % (room + 1)
    sizes = sizes.at[1:1 + 2 * couples:2].set(donor - moved).at[2:2 + 2 * couples:2].set(sink + moved)
    return sizes[jax.random.permutation(jax.random.fold_in(own_key, 2), amount)]


def bell_draw(stream_key, dims, spread, limit, shards=(), kind=jnp.bfloat16):
    entries = spread * jax.random.normal(stream_key, dims, jnp.float32)
    if shards:
        entries = entries * steps_of(stream_key, dims, shards, -0.22, 0.18)
    return jnp.clip(entries, -limit, limit).astype(kind)


def setup_inputs(seed: int = 0) -> dict:
    seeds = jax.random.split(jax.random.key(seed), 15)
    hidden_in = bell_draw(seeds[0], (SLOTS, TOK_MB, D), 1.0, 6.0, ((0, 8), (1, 4)))
    first_values = bell_draw(seeds[1], (SLOTS, D, TOK_MB), 1.0, 6.0, ((0, 8), (1, 4)))
    lengths = jax.vmap(lambda own: ragged(own, NSEQ, TOK_MB, LMAX, 2))(jax.random.split(seeds[2], SLOTS)).reshape((SLOTS, NSEQ)).astype(jnp.int32)
    places = jax.vmap(lambda own: jax.random.permutation(own, TOK_MB))(jax.random.split(seeds[3], SLOTS)).reshape((SLOTS, TOK_MB)).astype(jnp.int32)
    gain_attn = jnp.clip(1.0 + 0.18 * jax.random.normal(seeds[4], (D,), jnp.float32), 0.1, 1.9)
    gain_ffn = jnp.clip(1.0 + 0.18 * jax.random.normal(seeds[5], (D,), jnp.float32), 0.1, 1.9)
    w_query = bell_draw(seeds[6], (D, D), D ** -0.5, 0.1875, ((0, 8), (1, 4)))
    w_key = bell_draw(seeds[7], (D, D), D ** -0.5, 0.1875, ((0, 8), (1, 4)))
    w_value = bell_draw(seeds[8], (D, D), D ** -0.5, 0.1875, ((0, 8), (1, 4)))
    w_out = bell_draw(seeds[9], (D, D), 4 ** -0.5, 3.0, ((0, 4), (1, 8)))
    w_gate = bell_draw(seeds[10], (D, FF), D ** -0.5, 0.1875, ((0, 8), (1, 4)))
    w_up = bell_draw(seeds[11], (D, FF), D ** -0.5, 0.1875, ((0, 8), (1, 4)))
    w_down = bell_draw(seeds[12], (FF, D), FF ** -0.5, 0.109375, ((0, 4), (1, 8)))
    out_grad = bell_draw(seeds[13], (SLOTS, TOK_MB, D), 1.0, 6.0, ((0, 8), (1, 4)))
    return dict(hidden_in=hidden_in, first_values=first_values, lengths=lengths, places=places, gain_attn=gain_attn, gain_ffn=gain_ffn, w_query=w_query, w_key=w_key, w_value=w_value, w_out=w_out, w_gate=w_gate, w_up=w_up, w_down=w_down, out_grad=out_grad)


HIGHEST = lax.Precision.HIGHEST
EPSILON = 1e-06
MASKED = -1e+30

@jax.custom_vjp
def low(v):
    return lax.optimization_barrier(v.astype(jnp.bfloat16)).astype(jnp.float32)

@jax.custom_vjp
def low_back(v):
    return v

def low_keep(v):
    return (low(v), None)

def low_pass(kept, grad):
    return (grad,)

def back_keep(v):
    return (v, None)

def back_low(kept, grad):
    return (low(grad),)
low.defvjp(low_keep, low_pass)
low_back.defvjp(back_keep, back_low)

def product(left, right):
    return jnp.dot(left, right, precision=HIGHEST)

def token_places(lengths_row, count):
    ends_at = jnp.cumsum(lengths_row).astype(jnp.int32)
    index_row = jnp.arange(count, dtype=jnp.int32)
    segment_id = lax.optimization_barrier(jnp.sum((index_row[:, None] >= ends_at[None, :]).astype(jnp.int32), axis=1))
    starts_at = ends_at - lengths_row
    one_hot = segment_id[:, None] == jnp.arange(lengths_row.shape[0], dtype=jnp.int32)[None, :]
    position = index_row - lax.optimization_barrier(jnp.sum(jnp.where(one_hot, starts_at[None, :], 0), axis=1)).astype(jnp.int32)
    return (segment_id, position)

def rotary_tables(position):
    half_dim = HEAD_DIM // 2
    freq_index = jnp.arange(half_dim, dtype=jnp.float32)
    inverse = 10000.0 ** (-freq_index / half_dim)
    angles = position.astype(jnp.float32)[:, None] * inverse[None, :]
    return (jnp.cos(angles)[:, None, :], jnp.sin(angles)[:, None, :])

def rotate(field, cosine, sine):
    half_dim = field.shape[-1] // 2
    first_half, second_half = (field[..., :half_dim], field[..., half_dim:])
    return jnp.concatenate([first_half * cosine - second_half * sine, second_half * cosine + first_half * sine], axis=-1)

def rms_scale(field, gain):
    return field * lax.rsqrt(lax.optimization_barrier(jnp.mean(field * field, axis=-1, keepdims=True)) + EPSILON) * gain

def slot_forward(params, slot):
    gain_one, gain_two, w_query, w_key, w_value, w_out, w_gate, w_up, w_down = params
    stored_hidden, stored_first, lengths_row, places_row = slot
    count = stored_hidden.shape[0]
    packed_order = jnp.zeros((count,), jnp.int32).at[places_row].set(jnp.arange(count, dtype=jnp.int32))
    hidden_slot = jnp.take(stored_hidden, packed_order, axis=0)
    first_slot = jnp.take(stored_first, packed_order, axis=0)
    segment_id, position = token_places(lengths_row, count)
    cosine, sine = rotary_tables(position)
    score_scale = HEAD_DIM ** (-0.5)
    normed_one = low(rms_scale(hidden_slot, gain_one))
    query_raw = low_back(product(normed_one, w_query)).reshape(count, HEADS, HEAD_DIM)
    key_raw = low_back(product(normed_one, w_key)).reshape(count, HEADS, HEAD_DIM)
    queries = low(rotate(query_raw, cosine, sine))
    keys = low(rotate(key_raw, cosine, sine))
    values = low(low_back(0.5 * product(normed_one, w_value) + 0.5 * first_slot)).reshape(count, HEADS, HEAD_DIM)
    block_rows = min(512, count)
    token_index = jnp.arange(count, dtype=jnp.int32)

    def attend(block_index):
        start_row = (block_index * block_rows).astype(jnp.int32)
        query_block = lax.dynamic_slice_in_dim(queries, start_row, block_rows)
        query_seg = lax.dynamic_slice_in_dim(segment_id, start_row, block_rows)
        query_index = start_row + jnp.arange(block_rows, dtype=jnp.int32)
        allowed = (query_seg[:, None] == segment_id[None, :]) & (query_index[:, None] >= token_index[None, :])
        raw_scores = jnp.einsum('qhd,khd->hqk', query_block, keys, precision=HIGHEST)
        scores = jnp.where(allowed[None], low_back(score_scale * raw_scores), MASKED)
        log_total = jax.nn.logsumexp(scores, axis=-1, keepdims=True)
        probs = low(jnp.exp(scores - log_total))
        return jnp.einsum('hqk,khd->qhd', probs, values, precision=HIGHEST)
    blocks_out = lax.map(jax.checkpoint(attend), jnp.arange(count // block_rows, dtype=jnp.int32))
    attended = low(low_back(blocks_out.reshape(count, D)))
    mid = hidden_slot + low_back(product(attended, w_out))
    normed_two = low(rms_scale(mid, gain_two))
    gate_raw = low_back(product(normed_two, w_gate))
    up_raw = low_back(product(normed_two, w_up))
    hidden_act = low(jax.nn.silu(gate_raw) * up_raw)
    packed_out = mid + product(hidden_act, w_down)
    return jnp.take(packed_out, places_row, axis=0)

def reference(hidden_in, first_values, lengths, places, gain_attn, gain_ffn, w_query, w_key, w_value, w_out, w_gate, w_up, w_down, out_grad):
    primals = tuple((item.astype(jnp.float32) for item in (hidden_in, first_values, gain_attn, gain_ffn, w_query, w_key, w_value, w_out, w_gate, w_up, w_down)))

    def forward(hidden_all, first_all, gain_one, gain_two, wq_mat, wk_mat, wv_mat, wo_mat, wg_mat, wu_mat, wd_mat):
        params = (gain_one, gain_two, wq_mat, wk_mat, wv_mat, wo_mat, wg_mat, wu_mat, wd_mat)

        def slot_step(carry, slot):
            return (carry, jax.checkpoint(slot_forward)(params, slot))
        unused, outputs = lax.scan(slot_step, jnp.zeros((), jnp.float32), (hidden_all, jnp.transpose(first_all, (0, 2, 1)), lengths, places))
        return outputs
    output, pullback = jax.vjp(forward, *primals)
    grads = pullback(out_grad.astype(jnp.float32))
    return (output.astype(jnp.bfloat16), grads[0], grads[1], grads[2], grads[3], grads[4], grads[5], grads[6], grads[7], grads[8], grads[9], grads[10])
```

```python
import jax
import jax.numpy as jnp
from jax import lax
from jax.sharding import PartitionSpec as P

D = 1024
HEAD_DIM = 64
TOK_MB = 512
MICRO = 4


EPSILON = 1e-06
MASKED = -1e30


def product(left, right):
    return jnp.dot(left, right, preferred_element_type=jnp.float32)


def product_left(left, right):
    return lax.dot_general(
        left, right, (((0,), (0,)), ((), ())), preferred_element_type=jnp.float32
    )


def product_right(left, right):
    return lax.dot_general(
        left, right, (((1,), (1,)), ((), ())), preferred_element_type=jnp.float32
    )


def token_places(lengths_row, count):
    ends_at = jnp.cumsum(lengths_row)
    index_row = jnp.arange(count, dtype=jnp.int32)
    segment_id = jnp.sum((index_row[:, None] >= ends_at[None, :]).astype(jnp.int32), axis=1)
    starts_at = ends_at - lengths_row
    one_hot = segment_id[:, None] == jnp.arange(lengths_row.shape[0], dtype=jnp.int32)[None, :]
    position = index_row - jnp.sum(jnp.where(one_hot, starts_at[None, :], 0), axis=1)
    return (segment_id, position)


def rotary_tables(position):
    half_dim = HEAD_DIM // 2
    freq_index = jnp.arange(half_dim, dtype=jnp.float32)
    inverse = 10000.0 ** (-freq_index / half_dim)
    angles = position.astype(jnp.float32)[:, None] * inverse[None, :]
    return (jnp.cos(angles)[:, None, :], jnp.sin(angles)[:, None, :])


def rotate(field, cosine, sine):
    half_dim = field.shape[-1] // 2
    first_half, second_half = (field[..., :half_dim], field[..., half_dim:])
    return jnp.concatenate(
        [first_half * cosine - second_half * sine, second_half * cosine + first_half * sine],
        axis=-1,
    )


def rotate_back(field, cosine, sine):
    half_dim = field.shape[-1] // 2
    first_half, second_half = (field[..., :half_dim], field[..., half_dim:])
    return jnp.concatenate(
        [first_half * cosine + second_half * sine, second_half * cosine - first_half * sine],
        axis=-1,
    )


def spread_tokens(values):
    return lax.all_gather(values, "col", axis=0, tiled=True)


def reduce_tokens(values):
    return lax.psum_scatter(values, "col", scatter_dimension=0, tiled=True)


def tiled_body(
    hidden_in,
    first_values,
    lengths,
    places,
    gain_attn,
    gain_ffn,
    w_query,
    w_key,
    w_value,
    w_out,
    w_gate,
    w_up,
    w_down,
    out_grad,
):
    width_col = w_query.shape[1]
    heads_col = width_col // HEAD_DIM
    block_rows = min(512, TOK_MB)
    block_count = TOK_MB // block_rows
    local_rows = hidden_in.shape[1]
    row_start = lax.axis_index("col") * local_rows
    score_scale = HEAD_DIM ** (-0.5)
    tiles = (w_query, w_key, w_value, w_out, w_gate, w_up, w_down)

    def own_rows(values):
        return lax.dynamic_slice_in_dim(values, row_start, local_rows)

    hidden_width = w_gate.shape[1]
    full_shapes = (
        (D, width_col),
        (D, width_col),
        (D, width_col),
        (width_col, D),
        (D, hidden_width),
        (D, hidden_width),
        (hidden_width, D),
    )
    grads_full = tuple((jnp.zeros(shape_item, jnp.float32) for shape_item in full_shapes))
    grads_tile = tuple((jnp.zeros(tile_item.shape, jnp.float32) for tile_item in tiles))
    gain_sum_one = jnp.zeros((D,), jnp.float32)
    gain_sum_two = jnp.zeros((D,), jnp.float32)
    out_pieces, input_pieces, value_pieces = ([], [], [])
    for micro_step in range(MICRO):
        gathered = (
            lax.all_gather(tiles[0], "row", axis=0, tiled=True),
            lax.all_gather(tiles[1], "row", axis=0, tiled=True),
            lax.all_gather(tiles[2], "row", axis=0, tiled=True),
            lax.all_gather(tiles[3], "row", axis=1, tiled=True),
            lax.all_gather(tiles[4], "row", axis=0, tiled=True),
            lax.all_gather(tiles[5], "row", axis=0, tiled=True),
            lax.all_gather(tiles[6], "row", axis=1, tiled=True),
        )
        wq_all, wk_all, wv_all, wo_all, wg_all, wu_all, wd_all = gathered
        places_mb = places[micro_step]
        packed_order = (
            jnp.zeros((TOK_MB,), jnp.int32).at[places_mb].set(jnp.arange(TOK_MB, dtype=jnp.int32))
        )
        stored_hidden, stored_grad = (
            lax.all_gather(hidden_in[micro_step], "col", axis=0, tiled=True),
            lax.all_gather(out_grad[micro_step], "col", axis=0, tiled=True),
        )
        hidden_full = jnp.take(stored_hidden, packed_order, axis=0).astype(jnp.float32)
        grad_full_rows = jnp.take(stored_grad, packed_order, axis=0)
        first_mb = jnp.take(jnp.transpose(first_values[micro_step]), packed_order, axis=0).astype(
            jnp.float32
        )
        hidden_mb = own_rows(hidden_full)
        grad_mb = own_rows(grad_full_rows)
        segment_id, position = token_places(lengths[micro_step], TOK_MB)
        cosine, sine = rotary_tables(position)
        token_index = jnp.arange(TOK_MB, dtype=jnp.int32)
        scale_full = lax.rsqrt(jnp.mean(hidden_full * hidden_full, axis=1, keepdims=True) + EPSILON)
        scale_one = own_rows(scale_full)
        normed_one = (hidden_full * scale_full * gain_attn).astype(jnp.bfloat16)
        query_raw = product(normed_one, wq_all).reshape(TOK_MB, heads_col, HEAD_DIM)
        key_raw = product(normed_one, wk_all).reshape(TOK_MB, heads_col, HEAD_DIM)
        queries = rotate(query_raw, cosine, sine).astype(jnp.bfloat16)
        keys = rotate(key_raw, cosine, sine).astype(jnp.bfloat16)
        values = (
            (0.5 * product(normed_one, wv_all) + 0.5 * first_mb)
            .astype(jnp.bfloat16)
            .reshape(TOK_MB, heads_col, HEAD_DIM)
        )

        def block_scores(start_row):
            query_index = start_row + jnp.arange(block_rows, dtype=jnp.int32)
            allowed = (segment_id[:, None] == segment_id[None, :]) & (
                query_index[:, None] >= token_index[None, :]
            )
            raw_scores = (
                jnp.einsum("qhd,khd->hqk", queries, keys, preferred_element_type=jnp.float32)
                * score_scale
            )
            return (queries, jnp.where(allowed[None], raw_scores, MASKED))

        def attend(block_index):
            query_block, scores = block_scores(block_index * block_rows)
            row_top = jnp.max(scores, axis=-1, keepdims=True)
            log_total = row_top + jnp.log(
                jnp.sum(jnp.exp(scores - row_top), axis=-1, keepdims=True)
            )
            probs = jnp.exp(scores - log_total).astype(jnp.bfloat16)
            mixed = jnp.einsum("hqk,khd->qhd", probs, values, preferred_element_type=jnp.float32)
            return (mixed.astype(jnp.bfloat16), log_total[..., 0])

        attended, log_totals = lax.map(attend, jnp.arange(block_count, dtype=jnp.int32))
        attended = attended.reshape(TOK_MB, width_col)
        mid_mb = hidden_mb + reduce_tokens(product(attended, wo_all))
        scale_two = lax.rsqrt(jnp.mean(mid_mb * mid_mb, axis=1, keepdims=True) + EPSILON)
        normed_two = spread_tokens((mid_mb * scale_two * gain_ffn).astype(jnp.bfloat16))
        gate_raw = product(normed_two, wg_all)
        up_raw = product(normed_two, wu_all)
        sigmoid_gate = jax.nn.sigmoid(gate_raw)
        silu_gate = gate_raw * sigmoid_gate
        hidden_act = (silu_gate * up_raw).astype(jnp.bfloat16)
        packed_out = (mid_mb + reduce_tokens(product(hidden_act, wd_all))).astype(jnp.bfloat16)
        grad_down = product_left(hidden_act, grad_full_rows)
        d_hidden = product_right(grad_full_rows, wd_all)
        d_gate = (
            d_hidden * up_raw * sigmoid_gate * (1.0 + gate_raw * (1.0 - sigmoid_gate))
        ).astype(jnp.bfloat16)
        d_up = (d_hidden * silu_gate).astype(jnp.bfloat16)
        grad_gate = product_left(normed_two, d_gate)
        grad_up = product_left(normed_two, d_up)
        d_normed_two = reduce_tokens(product_right(d_gate, wg_all) + product_right(d_up, wu_all))
        gain_sum_two = gain_sum_two + jnp.sum(d_normed_two * mid_mb * scale_two, axis=0)
        scaled_two = d_normed_two * gain_ffn
        stat_two = jnp.sum(scaled_two * mid_mb, axis=1, keepdims=True)
        d_mid = (
            grad_mb.astype(jnp.float32)
            + scale_two * scaled_two
            - mid_mb * (scale_two * scale_two * scale_two * stat_two / D)
        )
        d_branch = spread_tokens(d_mid.astype(jnp.bfloat16))
        grad_out = product_left(attended, d_branch)
        d_attended = (
            product_right(d_branch, wo_all)
            .astype(jnp.bfloat16)
            .reshape(TOK_MB, heads_col, HEAD_DIM)
        )

        def attend_back(carry, block_index):
            key_acc, value_acc = carry
            start_row = block_index * block_rows
            query_block, scores = block_scores(start_row)
            log_block = log_totals[block_index]
            probs = jnp.exp(scores - log_block[..., None])
            d_probs = jnp.einsum(
                "qhd,khd->hqk", d_attended, values, preferred_element_type=jnp.float32
            )
            inner_sum = jnp.sum(probs * d_probs, axis=-1, keepdims=True)
            d_scores = (probs * (d_probs - inner_sum)).astype(jnp.bfloat16)
            d_query = (
                jnp.einsum("hqk,khd->qhd", d_scores, keys, preferred_element_type=jnp.float32)
                * score_scale
            )
            key_acc = (
                key_acc
                + jnp.einsum(
                    "hqk,qhd->khd", d_scores, query_block, preferred_element_type=jnp.float32
                )
                * score_scale
            )
            value_acc = value_acc + jnp.einsum(
                "hqk,qhd->khd",
                probs.astype(jnp.bfloat16),
                d_attended,
                preferred_element_type=jnp.float32,
            )
            return ((key_acc, value_acc), d_query)

        empty_heads = jnp.zeros((TOK_MB, heads_col, HEAD_DIM), jnp.float32)
        (key_grads, value_grads), query_grads = lax.scan(
            attend_back, (empty_heads, empty_heads), jnp.arange(block_count, dtype=jnp.int32)
        )
        d_values = value_grads.astype(jnp.bfloat16).reshape(TOK_MB, width_col)
        half_values = 0.5 * d_values.astype(jnp.float32)
        value_pieces.append(jnp.transpose(jnp.take(half_values, places_mb, axis=0)))
        d_value_proj = half_values.astype(jnp.bfloat16)
        d_query_raw = (
            rotate_back(query_grads.reshape(TOK_MB, heads_col, HEAD_DIM), cosine, sine)
            .astype(jnp.bfloat16)
            .reshape(TOK_MB, width_col)
        )
        d_key_raw = (
            rotate_back(key_grads, cosine, sine).astype(jnp.bfloat16).reshape(TOK_MB, width_col)
        )
        grad_query = product_left(normed_one, d_query_raw)
        grad_key = product_left(normed_one, d_key_raw)
        grad_value = product_left(normed_one, d_value_proj)
        d_normed_one = reduce_tokens(
            product_right(d_query_raw, wq_all)
            + product_right(d_key_raw, wk_all)
            + product_right(d_value_proj, wv_all)
        )
        gain_sum_one = gain_sum_one + jnp.sum(d_normed_one * hidden_mb * scale_one, axis=0)
        scaled_one = d_normed_one * gain_attn
        stat_one = jnp.sum(scaled_one * hidden_mb, axis=1, keepdims=True)
        packed_input = (
            d_mid
            + scale_one * scaled_one
            - hidden_mb * (scale_one * scale_one * scale_one * stat_one / D)
        )
        out_whole, input_whole = (
            lax.all_gather(
                packed_out.astype(jnp.float32).astype(jnp.bfloat16), "col", axis=0, tiled=True
            ).astype(jnp.float32),
            lax.all_gather(packed_input.astype(jnp.bfloat16), "col", axis=0, tiled=True).astype(
                packed_input.dtype
            ),
        )
        stored_places = lax.dynamic_slice_in_dim(places_mb, row_start, local_rows)
        out_pieces.append(jnp.take(out_whole, stored_places, axis=0).astype(jnp.bfloat16))
        input_pieces.append(jnp.take(input_whole, stored_places, axis=0))
        new_grads = (grad_query, grad_key, grad_value, grad_out, grad_gate, grad_up, grad_down)
        grads_full = tuple((earlier + later for earlier, later in zip(grads_full, new_grads)))
    grads_tile = (
        lax.psum_scatter(
            grads_full[0].astype(jnp.bfloat16), "row", scatter_dimension=0, tiled=True
        ).astype(jnp.float32),
        lax.psum_scatter(
            grads_full[1].astype(jnp.bfloat16), "row", scatter_dimension=0, tiled=True
        ).astype(jnp.float32),
        lax.psum_scatter(
            grads_full[2].astype(jnp.bfloat16), "row", scatter_dimension=0, tiled=True
        ).astype(jnp.float32),
        lax.psum_scatter(
            grads_full[3].astype(jnp.bfloat16), "row", scatter_dimension=1, tiled=True
        ).astype(jnp.float32),
        lax.psum_scatter(
            grads_full[4].astype(jnp.bfloat16), "row", scatter_dimension=0, tiled=True
        ).astype(jnp.float32),
        lax.psum_scatter(
            grads_full[5].astype(jnp.bfloat16), "row", scatter_dimension=0, tiled=True
        ).astype(jnp.float32),
        lax.psum_scatter(
            grads_full[6].astype(jnp.bfloat16), "row", scatter_dimension=1, tiled=True
        ).astype(jnp.float32),
    )
    gain_grad_one, gain_grad_two = lax.psum((gain_sum_one, gain_sum_two), ("row", "col"))
    return (
        jnp.stack(out_pieces, axis=0),
        jnp.stack(input_pieces, axis=0),
        jnp.stack(value_pieces, axis=0),
        gain_grad_one,
        gain_grad_two,
        grads_tile[0],
        grads_tile[1],
        grads_tile[2],
        grads_tile[3],
        grads_tile[4],
        grads_tile[5],
        grads_tile[6],
    )


def slot_body(
    hidden_in,
    first_values,
    lengths,
    places,
    gain_attn,
    gain_ffn,
    w_query,
    w_key,
    w_value,
    w_out,
    w_gate,
    w_up,
    w_down,
    out_grad,
):
    slots, rows, width = hidden_in.shape
    count = slots * rows
    heads = width // HEAD_DIM
    hidden_tile = w_gate.shape[1]
    column = lax.axis_index("col")
    score_scale = HEAD_DIM ** (-0.5)
    both = ("row", "col")

    def gather(tile):
        return lax.all_gather(tile, both, axis=0, tiled=False)

    row_count = width // w_query.shape[0]

    def by_rows(whole, count_out):
        tile_rows, tile_cols = whole.shape[1:]
        whole = whole.reshape(row_count, slots, tile_rows, tile_cols)
        return jnp.transpose(whole, (0, 2, 1, 3)).reshape(row_count * tile_rows, count_out)

    def by_cols(whole, count_in):
        tile_rows, tile_cols = whole.shape[1:]
        whole = whole.reshape(row_count, slots, tile_rows, tile_cols)
        return jnp.transpose(whole, (1, 2, 0, 3)).reshape(count_in, row_count * tile_cols)

    ff = hidden_tile * slots
    wide = w_query.shape[1]
    qkv_tiles = gather(jnp.concatenate([w_query, w_key, w_value], axis=1))
    wq = by_rows(qkv_tiles[:, :, :wide], width)
    wk = by_rows(qkv_tiles[:, :, wide : 2 * wide], width)
    wv = by_rows(qkv_tiles[:, :, 2 * wide :], width)
    wo = by_cols(gather(w_out), width)
    wg = by_rows(gather(w_gate), ff)
    wu = by_rows(gather(w_up), ff)
    wd = by_cols(gather(w_down), ff)

    first_rows = jnp.transpose(first_values, (0, 2, 1))
    feature_tile = first_rows.shape[2]
    first_packed = first_rows.reshape(slots, slots, rows, feature_tile)
    first_packed = jnp.transpose(first_packed, (0, 2, 1, 3)).reshape(slots, rows, width)
    sent = jnp.concatenate([hidden_in, out_grad, first_packed], axis=1)
    got = lax.all_to_all(sent, "col", split_axis=0, concat_axis=0, tiled=True)
    hidden = got[:, :rows].reshape(count, width).astype(jnp.float32)
    grad_rows = got[:, rows : 2 * rows].reshape(count, width)
    first = got[:, 2 * rows :].reshape(slots, rows, slots, feature_tile)
    first = jnp.transpose(first, (2, 1, 0, 3)).reshape(count, width).astype(jnp.float32)

    place = lax.dynamic_index_in_dim(places, column, 0, keepdims=False)
    length = lax.dynamic_index_in_dim(lengths, column, 0, keepdims=False)
    ends_at = jnp.cumsum(length)
    starts_at = ends_at - length
    past = place[:, None] >= ends_at[None, :]
    segment_id = jnp.sum(past.astype(jnp.int32), axis=1)
    one_hot = segment_id[:, None] == jnp.arange(length.shape[0], dtype=jnp.int32)[None, :]
    position = place - jnp.sum(jnp.where(one_hot, starts_at[None, :], 0), axis=1)
    cosine, sine = rotary_tables(position)
    allowed = (segment_id[:, None] == segment_id[None, :]) & (place[:, None] >= place[None, :])

    scale_one = lax.rsqrt(jnp.mean(hidden * hidden, axis=1, keepdims=True) + EPSILON)
    normed_one = (hidden * scale_one * gain_attn).astype(jnp.bfloat16)
    by_head = (count, heads, HEAD_DIM)
    queries = rotate(product(normed_one, wq).reshape(by_head), cosine, sine).astype(jnp.bfloat16)
    keys = rotate(product(normed_one, wk).reshape(by_head), cosine, sine).astype(jnp.bfloat16)
    values = (0.5 * product(normed_one, wv) + 0.5 * first).astype(jnp.bfloat16).reshape(by_head)

    raw_scores = jnp.einsum("qhd,khd->hqk", queries, keys, preferred_element_type=jnp.float32)
    scores = jnp.where(allowed[None], raw_scores * score_scale, MASKED)
    row_top = jnp.max(scores, axis=-1, keepdims=True)
    log_total = row_top + jnp.log(jnp.sum(jnp.exp(scores - row_top), axis=-1, keepdims=True))
    probs = jnp.exp(scores - log_total)
    probs_low = probs.astype(jnp.bfloat16)
    attended = (
        jnp.einsum("hqk,khd->qhd", probs_low, values, preferred_element_type=jnp.float32)
        .astype(jnp.bfloat16)
        .reshape(count, width)
    )
    mid = hidden + product(attended, wo)
    scale_two = lax.rsqrt(jnp.mean(mid * mid, axis=1, keepdims=True) + EPSILON)
    normed_two = (mid * scale_two * gain_ffn).astype(jnp.bfloat16)
    gate_raw = product(normed_two, wg)
    up_raw = product(normed_two, wu)
    sigmoid_gate = jax.nn.sigmoid(gate_raw)
    silu_gate = gate_raw * sigmoid_gate
    hidden_act = (silu_gate * up_raw).astype(jnp.bfloat16)
    stored_out = (mid + product(hidden_act, wd)).astype(jnp.bfloat16)

    def scatter(tiles):
        tiles = tiles.reshape((row_count * slots,) + tiles.shape[2:])
        return lax.psum_scatter(tiles, both, scatter_dimension=0, tiled=False).astype(jnp.float32)

    def tiles_by_rows(grad):
        depth, across = grad.shape
        grad = grad.astype(jnp.bfloat16)
        grad = grad.reshape(row_count, depth // row_count, slots, across // slots)
        return scatter(jnp.transpose(grad, (0, 2, 1, 3)))

    def tiles_by_cols(grad):
        depth, across = grad.shape
        grad = grad.astype(jnp.bfloat16)
        grad = grad.reshape(slots, depth // slots, row_count, across // row_count)
        return scatter(jnp.transpose(grad, (2, 0, 1, 3)))

    grad_down = tiles_by_cols(product_left(hidden_act, grad_rows))
    d_hidden = product_right(grad_rows, wd)
    d_gate = (d_hidden * up_raw * sigmoid_gate * (1.0 + gate_raw * (1.0 - sigmoid_gate))).astype(
        jnp.bfloat16
    )
    d_up = (d_hidden * silu_gate).astype(jnp.bfloat16)
    grad_gate = tiles_by_rows(product_left(normed_two, d_gate))
    grad_up = tiles_by_rows(product_left(normed_two, d_up))
    d_normed_two = product_right(d_gate, wg) + product_right(d_up, wu)
    gain_sum_two = jnp.sum(d_normed_two * mid * scale_two, axis=0)
    scaled_two = d_normed_two * gain_ffn
    stat_two = jnp.sum(scaled_two * mid, axis=1, keepdims=True)
    d_mid = (
        grad_rows.astype(jnp.float32)
        + scale_two * scaled_two
        - mid * (scale_two * scale_two * scale_two * stat_two / width)
    )
    d_branch = d_mid.astype(jnp.bfloat16)
    grad_out = tiles_by_cols(product_left(attended, d_branch))
    d_attended = product_right(d_branch, wo).astype(jnp.bfloat16).reshape(by_head)
    d_probs = jnp.einsum("qhd,khd->hqk", d_attended, values, preferred_element_type=jnp.float32)
    inner_sum = jnp.sum(probs * d_probs, axis=-1, keepdims=True)
    d_scores = (probs * (d_probs - inner_sum)).astype(jnp.bfloat16)
    d_query = score_scale * jnp.einsum(
        "hqk,khd->qhd", d_scores, keys, preferred_element_type=jnp.float32
    )
    d_key = score_scale * jnp.einsum(
        "hqk,qhd->khd", d_scores, queries, preferred_element_type=jnp.float32
    )
    d_values = (
        jnp.einsum("hqk,qhd->khd", probs_low, d_attended, preferred_element_type=jnp.float32)
        .astype(jnp.bfloat16)
        .reshape(count, width)
    )
    d_value_proj = (0.5 * d_values.astype(jnp.float32)).astype(jnp.bfloat16)
    d_query_raw = rotate_back(d_query, cosine, sine).astype(jnp.bfloat16).reshape(count, width)
    d_key_raw = rotate_back(d_key, cosine, sine).astype(jnp.bfloat16).reshape(count, width)
    grad_query = tiles_by_rows(product_left(normed_one, d_query_raw))
    grad_key = tiles_by_rows(product_left(normed_one, d_key_raw))
    grad_value = tiles_by_rows(product_left(normed_one, d_value_proj))
    d_normed_one = (
        product_right(d_query_raw, wq)
        + product_right(d_key_raw, wk)
        + product_right(d_value_proj, wv)
    )
    gain_sum_one = jnp.sum(d_normed_one * hidden * scale_one, axis=0)
    scaled_one = d_normed_one * gain_attn
    stat_one = jnp.sum(scaled_one * hidden, axis=1, keepdims=True)
    input_grad = (
        d_mid
        + scale_one * scaled_one
        - hidden * (scale_one * scale_one * scale_one * stat_one / width)
    )
    value_sent = d_value_proj.reshape(slots, rows, slots, feature_tile)
    value_sent = jnp.transpose(value_sent, (2, 1, 0, 3)).reshape(slots, rows, width)
    sent_back = jnp.concatenate(
        [
            stored_out.reshape(slots, rows, width),
            input_grad.astype(jnp.bfloat16).reshape(slots, rows, width),
            value_sent,
        ],
        axis=1,
    )
    back = lax.all_to_all(sent_back, "col", split_axis=0, concat_axis=0, tiled=True)
    value_back = back[:, 2 * rows :].reshape(slots, rows, slots, feature_tile)
    value_back = jnp.transpose(value_back, (0, 3, 2, 1)).reshape(slots, feature_tile, count)
    gain_grad_one, gain_grad_two = lax.psum((gain_sum_one, gain_sum_two), both)
    return (
        back[:, :rows],
        back[:, rows : 2 * rows].astype(jnp.float32),
        value_back.astype(jnp.float32),
        gain_grad_one,
        gain_grad_two,
        grad_query,
        grad_key,
        grad_value,
        grad_out,
        grad_gate,
        grad_up,
        grad_down,
    )


def solution(mesh):
    def body(*arrays):
        one_each = arrays[0].shape[0] == mesh.shape["col"]
        return (slot_body if one_each else tiled_body)(*arrays)

    return jax.shard_map(
        body,
        mesh=mesh,
        in_specs=(
            P("row", "col", None),
            P("row", "col", None),
            P("row", None),
            P("row", None),
            P(),
            P(),
            P("row", "col"),
            P("row", "col"),
            P("row", "col"),
            P("col", "row"),
            P("row", "col"),
            P("row", "col"),
            P("col", "row"),
            P("row", "col", None),
        ),
        out_specs=(
            P("row", "col", None),
            P("row", "col", None),
            P("row", "col", None),
            P(),
            P(),
            P("row", "col"),
            P("row", "col"),
            P("row", "col"),
            P("col", "row"),
            P("row", "col"),
            P("row", "col"),
            P("col", "row"),
        ),
        check_vma=False,
    )
```

```python
import jax
import jax.numpy as jnp
from jax import lax
from jax.experimental import pallas as pl
from jax.experimental.pallas import tpu as pltpu
from jax.sharding import PartitionSpec as P

D = 1024
HEAD_DIM = 64
TOK_MB = 512
MICRO = 4


EPSILON = 1e-06
MASKED = -1e30


def product(left, right):
    return jnp.dot(left, right, preferred_element_type=jnp.float32)


def product_left(left, right):
    return lax.dot_general(
        left, right, (((0,), (0,)), ((), ())), preferred_element_type=jnp.float32
    )


def product_right(left, right):
    return lax.dot_general(
        left, right, (((1,), (1,)), ((), ())), preferred_element_type=jnp.float32
    )


def token_places(lengths_row, count):
    ends_at = jnp.cumsum(lengths_row)
    index_row = jnp.arange(count, dtype=jnp.int32)
    segment_id = jnp.sum((index_row[:, None] >= ends_at[None, :]).astype(jnp.int32), axis=1)
    starts_at = ends_at - lengths_row
    one_hot = segment_id[:, None] == jnp.arange(lengths_row.shape[0], dtype=jnp.int32)[None, :]
    position = index_row - jnp.sum(jnp.where(one_hot, starts_at[None, :], 0), axis=1)
    return (segment_id, position)


def rotary_tables(position):
    half_dim = HEAD_DIM // 2
    freq_index = jnp.arange(half_dim, dtype=jnp.float32)
    inverse = 10000.0 ** (-freq_index / half_dim)
    angles = position.astype(jnp.float32)[:, None] * inverse[None, :]
    return (jnp.cos(angles)[:, None, :], jnp.sin(angles)[:, None, :])


def rotate(field, cosine, sine):
    half_dim = field.shape[-1] // 2
    first_half, second_half = (field[..., :half_dim], field[..., half_dim:])
    return jnp.concatenate(
        [first_half * cosine - second_half * sine, second_half * cosine + first_half * sine],
        axis=-1,
    )


def rotate_back(field, cosine, sine):
    half_dim = field.shape[-1] // 2
    first_half, second_half = (field[..., :half_dim], field[..., half_dim:])
    return jnp.concatenate(
        [first_half * cosine + second_half * sine, second_half * cosine - first_half * sine],
        axis=-1,
    )


def spread_tokens(values):
    return lax.all_gather(values, "col", axis=0, tiled=True)


def reduce_tokens(values):
    return lax.psum_scatter(values, "col", scatter_dimension=0, tiled=True)


def tiled_body(
    hidden_in,
    first_values,
    lengths,
    places,
    gain_attn,
    gain_ffn,
    w_query,
    w_key,
    w_value,
    w_out,
    w_gate,
    w_up,
    w_down,
    out_grad,
):
    width_col = w_query.shape[1]
    heads_col = width_col // HEAD_DIM
    block_rows = min(512, TOK_MB)
    block_count = TOK_MB // block_rows
    local_rows = hidden_in.shape[1]
    row_start = lax.axis_index("col") * local_rows
    score_scale = HEAD_DIM ** (-0.5)
    tiles = (w_query, w_key, w_value, w_out, w_gate, w_up, w_down)

    def own_rows(values):
        return lax.dynamic_slice_in_dim(values, row_start, local_rows)

    hidden_width = w_gate.shape[1]
    full_shapes = (
        (D, width_col),
        (D, width_col),
        (D, width_col),
        (width_col, D),
        (D, hidden_width),
        (D, hidden_width),
        (hidden_width, D),
    )
    grads_full = tuple((jnp.zeros(shape_item, jnp.float32) for shape_item in full_shapes))
    grads_tile = tuple((jnp.zeros(tile_item.shape, jnp.float32) for tile_item in tiles))
    gain_sum_one = jnp.zeros((D,), jnp.float32)
    gain_sum_two = jnp.zeros((D,), jnp.float32)
    out_pieces, input_pieces, value_pieces = ([], [], [])
    for micro_step in range(MICRO):
        gathered = (
            lax.all_gather(tiles[0], "row", axis=0, tiled=True),
            lax.all_gather(tiles[1], "row", axis=0, tiled=True),
            lax.all_gather(tiles[2], "row", axis=0, tiled=True),
            lax.all_gather(tiles[3], "row", axis=1, tiled=True),
            lax.all_gather(tiles[4], "row", axis=0, tiled=True),
            lax.all_gather(tiles[5], "row", axis=0, tiled=True),
            lax.all_gather(tiles[6], "row", axis=1, tiled=True),
        )
        wq_all, wk_all, wv_all, wo_all, wg_all, wu_all, wd_all = gathered
        places_mb = places[micro_step]
        packed_order = (
            jnp.zeros((TOK_MB,), jnp.int32).at[places_mb].set(jnp.arange(TOK_MB, dtype=jnp.int32))
        )
        stored_hidden, stored_grad = (
            lax.all_gather(hidden_in[micro_step], "col", axis=0, tiled=True),
            lax.all_gather(out_grad[micro_step], "col", axis=0, tiled=True),
        )
        hidden_full = jnp.take(stored_hidden, packed_order, axis=0).astype(jnp.float32)
        grad_full_rows = jnp.take(stored_grad, packed_order, axis=0)
        first_mb = jnp.take(jnp.transpose(first_values[micro_step]), packed_order, axis=0).astype(
            jnp.float32
        )
        hidden_mb = own_rows(hidden_full)
        grad_mb = own_rows(grad_full_rows)
        segment_id, position = token_places(lengths[micro_step], TOK_MB)
        cosine, sine = rotary_tables(position)
        token_index = jnp.arange(TOK_MB, dtype=jnp.int32)
        scale_full = lax.rsqrt(jnp.mean(hidden_full * hidden_full, axis=1, keepdims=True) + EPSILON)
        scale_one = own_rows(scale_full)
        normed_one = (hidden_full * scale_full * gain_attn).astype(jnp.bfloat16)
        query_raw = product(normed_one, wq_all).reshape(TOK_MB, heads_col, HEAD_DIM)
        key_raw = product(normed_one, wk_all).reshape(TOK_MB, heads_col, HEAD_DIM)
        queries = rotate(query_raw, cosine, sine).astype(jnp.bfloat16)
        keys = rotate(key_raw, cosine, sine).astype(jnp.bfloat16)
        values = (
            (0.5 * product(normed_one, wv_all) + 0.5 * first_mb)
            .astype(jnp.bfloat16)
            .reshape(TOK_MB, heads_col, HEAD_DIM)
        )

        def block_scores(start_row):
            query_index = start_row + jnp.arange(block_rows, dtype=jnp.int32)
            allowed = (segment_id[:, None] == segment_id[None, :]) & (
                query_index[:, None] >= token_index[None, :]
            )
            raw_scores = (
                jnp.einsum("qhd,khd->hqk", queries, keys, preferred_element_type=jnp.float32)
                * score_scale
            )
            return (queries, jnp.where(allowed[None], raw_scores, MASKED))

        def attend(block_index):
            query_block, scores = block_scores(block_index * block_rows)
            row_top = jnp.max(scores, axis=-1, keepdims=True)
            log_total = row_top + jnp.log(
                jnp.sum(jnp.exp(scores - row_top), axis=-1, keepdims=True)
            )
            probs = jnp.exp(scores - log_total).astype(jnp.bfloat16)
            mixed = jnp.einsum("hqk,khd->qhd", probs, values, preferred_element_type=jnp.float32)
            return (mixed.astype(jnp.bfloat16), log_total[..., 0])

        attended, log_totals = lax.map(attend, jnp.arange(block_count, dtype=jnp.int32))
        attended = attended.reshape(TOK_MB, width_col)
        mid_mb = hidden_mb + reduce_tokens(product(attended, wo_all))
        scale_two = lax.rsqrt(jnp.mean(mid_mb * mid_mb, axis=1, keepdims=True) + EPSILON)
        normed_two = spread_tokens((mid_mb * scale_two * gain_ffn).astype(jnp.bfloat16))
        gate_raw = product(normed_two, wg_all)
        up_raw = product(normed_two, wu_all)
        sigmoid_gate = jax.nn.sigmoid(gate_raw)
        silu_gate = gate_raw * sigmoid_gate
        hidden_act = (silu_gate * up_raw).astype(jnp.bfloat16)
        packed_out = (mid_mb + reduce_tokens(product(hidden_act, wd_all))).astype(jnp.bfloat16)
        grad_down = product_left(hidden_act, grad_full_rows)
        d_hidden = product_right(grad_full_rows, wd_all)
        d_gate = (
            d_hidden * up_raw * sigmoid_gate * (1.0 + gate_raw * (1.0 - sigmoid_gate))
        ).astype(jnp.bfloat16)
        d_up = (d_hidden * silu_gate).astype(jnp.bfloat16)
        grad_gate = product_left(normed_two, d_gate)
        grad_up = product_left(normed_two, d_up)
        d_normed_two = reduce_tokens(product_right(d_gate, wg_all) + product_right(d_up, wu_all))
        gain_sum_two = gain_sum_two + jnp.sum(d_normed_two * mid_mb * scale_two, axis=0)
        scaled_two = d_normed_two * gain_ffn
        stat_two = jnp.sum(scaled_two * mid_mb, axis=1, keepdims=True)
        d_mid = (
            grad_mb.astype(jnp.float32)
            + scale_two * scaled_two
            - mid_mb * (scale_two * scale_two * scale_two * stat_two / D)
        )
        d_branch = spread_tokens(d_mid.astype(jnp.bfloat16))
        grad_out = product_left(attended, d_branch)
        d_attended = (
            product_right(d_branch, wo_all)
            .astype(jnp.bfloat16)
            .reshape(TOK_MB, heads_col, HEAD_DIM)
        )

        def attend_back(carry, block_index):
            key_acc, value_acc = carry
            start_row = block_index * block_rows
            query_block, scores = block_scores(start_row)
            log_block = log_totals[block_index]
            probs = jnp.exp(scores - log_block[..., None])
            d_probs = jnp.einsum(
                "qhd,khd->hqk", d_attended, values, preferred_element_type=jnp.float32
            )
            inner_sum = jnp.sum(probs * d_probs, axis=-1, keepdims=True)
            d_scores = (probs * (d_probs - inner_sum)).astype(jnp.bfloat16)
            d_query = (
                jnp.einsum("hqk,khd->qhd", d_scores, keys, preferred_element_type=jnp.float32)
                * score_scale
            )
            key_acc = (
                key_acc
                + jnp.einsum(
                    "hqk,qhd->khd", d_scores, query_block, preferred_element_type=jnp.float32
                )
                * score_scale
            )
            value_acc = value_acc + jnp.einsum(
                "hqk,qhd->khd",
                probs.astype(jnp.bfloat16),
                d_attended,
                preferred_element_type=jnp.float32,
            )
            return ((key_acc, value_acc), d_query)

        empty_heads = jnp.zeros((TOK_MB, heads_col, HEAD_DIM), jnp.float32)
        (key_grads, value_grads), query_grads = lax.scan(
            attend_back, (empty_heads, empty_heads), jnp.arange(block_count, dtype=jnp.int32)
        )
        d_values = value_grads.astype(jnp.bfloat16).reshape(TOK_MB, width_col)
        half_values = 0.5 * d_values.astype(jnp.float32)
        value_pieces.append(jnp.transpose(jnp.take(half_values, places_mb, axis=0)))
        d_value_proj = half_values.astype(jnp.bfloat16)
        d_query_raw = (
            rotate_back(query_grads.reshape(TOK_MB, heads_col, HEAD_DIM), cosine, sine)
            .astype(jnp.bfloat16)
            .reshape(TOK_MB, width_col)
        )
        d_key_raw = (
            rotate_back(key_grads, cosine, sine).astype(jnp.bfloat16).reshape(TOK_MB, width_col)
        )
        grad_query = product_left(normed_one, d_query_raw)
        grad_key = product_left(normed_one, d_key_raw)
        grad_value = product_left(normed_one, d_value_proj)
        d_normed_one = reduce_tokens(
            product_right(d_query_raw, wq_all)
            + product_right(d_key_raw, wk_all)
            + product_right(d_value_proj, wv_all)
        )
        gain_sum_one = gain_sum_one + jnp.sum(d_normed_one * hidden_mb * scale_one, axis=0)
        scaled_one = d_normed_one * gain_attn
        stat_one = jnp.sum(scaled_one * hidden_mb, axis=1, keepdims=True)
        packed_input = (
            d_mid
            + scale_one * scaled_one
            - hidden_mb * (scale_one * scale_one * scale_one * stat_one / D)
        )
        out_whole, input_whole = (
            lax.all_gather(
                packed_out.astype(jnp.float32).astype(jnp.bfloat16), "col", axis=0, tiled=True
            ).astype(jnp.float32),
            lax.all_gather(packed_input.astype(jnp.bfloat16), "col", axis=0, tiled=True).astype(
                packed_input.dtype
            ),
        )
        stored_places = lax.dynamic_slice_in_dim(places_mb, row_start, local_rows)
        out_pieces.append(jnp.take(out_whole, stored_places, axis=0).astype(jnp.bfloat16))
        input_pieces.append(jnp.take(input_whole, stored_places, axis=0))
        new_grads = (grad_query, grad_key, grad_value, grad_out, grad_gate, grad_up, grad_down)
        grads_full = tuple((earlier + later for earlier, later in zip(grads_full, new_grads)))
    grads_tile = (
        lax.psum_scatter(
            grads_full[0].astype(jnp.bfloat16), "row", scatter_dimension=0, tiled=True
        ).astype(jnp.float32),
        lax.psum_scatter(
            grads_full[1].astype(jnp.bfloat16), "row", scatter_dimension=0, tiled=True
        ).astype(jnp.float32),
        lax.psum_scatter(
            grads_full[2].astype(jnp.bfloat16), "row", scatter_dimension=0, tiled=True
        ).astype(jnp.float32),
        lax.psum_scatter(
            grads_full[3].astype(jnp.bfloat16), "row", scatter_dimension=1, tiled=True
        ).astype(jnp.float32),
        lax.psum_scatter(
            grads_full[4].astype(jnp.bfloat16), "row", scatter_dimension=0, tiled=True
        ).astype(jnp.float32),
        lax.psum_scatter(
            grads_full[5].astype(jnp.bfloat16), "row", scatter_dimension=0, tiled=True
        ).astype(jnp.float32),
        lax.psum_scatter(
            grads_full[6].astype(jnp.bfloat16), "row", scatter_dimension=1, tiled=True
        ).astype(jnp.float32),
    )
    gain_grad_one, gain_grad_two = lax.psum((gain_sum_one, gain_sum_two), ("row", "col"))
    return (
        jnp.stack(out_pieces, axis=0),
        jnp.stack(input_pieces, axis=0),
        jnp.stack(value_pieces, axis=0),
        gain_grad_one,
        gain_grad_two,
        grads_tile[0],
        grads_tile[1],
        grads_tile[2],
        grads_tile[3],
        grads_tile[4],
        grads_tile[5],
        grads_tile[6],
    )


MESH_IDS = pl.DeviceIdType.MESH
Z_SIZE = 4
FIRST_X = (0, 3)


def chip_coordinates():
    row, col = lax.axis_index("row"), lax.axis_index("col")
    return row // 2, row % 2, col // 2, col % 2


def device_of(z, x, y, core):
    return (z * 2 + x, y * 2 + core)


def greet(z, x, y, core):
    barrier = pltpu.get_barrier_semaphore()

    def signal(target):
        pl.semaphore_signal(barrier, inc=1, device_id=target, device_id_type=MESH_IDS)

    signal(device_of(z, 1 - x, y, core))
    signal(device_of(z, x, 1 - y, core))
    signal(device_of(z, x, y, 1 - core))

    for step in range(1, Z_SIZE):
        signal(device_of((z + step) % Z_SIZE, x, y, core))
    pl.semaphore_wait(barrier, 3 + Z_SIZE - 1)


def gather_kernel(*refs):
    count = len(FIRST_X) + 2
    shards, wholes = refs[:count], refs[count : 2 * count]
    own_sem, link_recv, core_recv, send_sem = refs[2 * count :]
    z, x, y, core = chip_coordinates()
    greet(z, x, y, core)

    def spot(array, pz, px, py, pcore):
        return wholes[array].at[py * 2 + pcore, :, pl.ds((pz * 2 + px) * 128, 128)]

    def chip_id(pz, px, py):
        return (pz * 2 + px) * 2 + py

    def link(array, pz, px, py, way, target, own=False):
        src = shards[array] if own else spot(array, pz, px, py, core)
        return pltpu.make_async_remote_copy(
            src_ref=src,
            dst_ref=spot(array, pz, px, py, core),
            send_sem=send_sem.at[array, way, chip_id(pz, px, py)],
            recv_sem=link_recv.at[array, chip_id(pz, px, py)],
            device_id=target,
            device_id_type=MESH_IDS,
        )

    def twin(array, pz, px, py, own=False):
        src = shards[array] if own else spot(array, pz, px, py, core)
        return pltpu.make_async_remote_copy(
            src_ref=src,
            dst_ref=spot(array, pz, px, py, core),
            send_sem=send_sem.at[array, 4, chip_id(pz, px, py)],
            recv_sem=core_recv.at[array, chip_id(pz, px, py)],
            device_id=device_of(z, x, y, 1 - core),
            device_id_type=MESH_IDS,
        )

    x_mate, y_mate = device_of(z, 1 - x, y, core), device_of(z, x, 1 - y, core)
    up, down = device_of(z + 1, x, y, core), device_of(z - 1, x, y, core)

    def across(array, pz, px, py, leg, own=False):
        if (array in FIRST_X) == (leg == 0):
            return link(array, pz, px, py, 2, x_mate, own)
        return link(array, pz, px, py, 3, y_mate, own)

    order = (0, 1, 2, 3)
    place_own = []
    for array in order:
        keep = pltpu.make_async_copy(shards[array], spot(array, z, x, y, core), own_sem.at[array])
        keep.start()
        place_own.append(keep)

        @pl.when(z < Z_SIZE - 1)
        def _():
            link(array, z, x, y, 0, up, True).start()

        @pl.when(z > 0)
        def _():
            link(array, z, x, y, 1, down, True).start()

        across(array, z, x, y, 0, True).start()
        twin(array, z, x, y, True).start()

    def second(array, pz):
        if array in FIRST_X:
            arrived, onward = (1 - x, y), (3, y_mate)
        else:
            arrived, onward = (x, 1 - y), (2, x_mate)
        moved = link(array, pz, *arrived, *onward)
        moved.wait_recv()
        moved.start()
        twin(array, pz, *arrived).start()

    def second_own(array, pz, own):
        across(array, pz, x, y, 1, own).start()

    for array in order:
        second_own(array, z, True)
        second(array, z)
    for step in range(1, Z_SIZE):
        for array in order:

            @pl.when(z >= step)
            def _():
                pz = z - step
                link(array, pz, x, y, 0, up).wait_recv()

                @pl.when(z < Z_SIZE - 1)
                def _():
                    link(array, pz, x, y, 0, up).start()

                across(array, pz, x, y, 0).start()
                twin(array, pz, x, y).start()

            @pl.when(z + step <= Z_SIZE - 1)
            def _():
                pz = z + step
                link(array, pz, x, y, 1, down).wait_recv()

                @pl.when(z > 0)
                def _():
                    link(array, pz, x, y, 1, down).start()

                across(array, pz, x, y, 0).start()
                twin(array, pz, x, y).start()

        for array in order:

            @pl.when(z >= step)
            def _():
                second_own(array, z - step, False)
                second(array, z - step)

            @pl.when(z + step <= Z_SIZE - 1)
            def _():
                second_own(array, z + step, False)
                second(array, z + step)

    def last(array, pz):
        far = ((x, 1 - y), (1 - x, 1 - y)) if array in FIRST_X else ((1 - x, y), (1 - x, 1 - y))
        for px, py in far:
            link(array, pz, px, py, 2, x_mate).wait_recv()
            twin(array, pz, px, py).start()

    for array in order:
        for pz in range(Z_SIZE):
            last(array, pz)
    for array in order:
        place_own[array].wait()
        for pz in range(Z_SIZE):
            for px in range(2):
                for py in range(2):
                    twin(array, pz, px, py).wait()
            link(array, pz, x, y, 2, x_mate).wait_send()
            link(array, pz, x, y, 3, y_mate).wait_send()
            if array in FIRST_X:
                link(array, pz, 1 - x, y, 3, y_mate).wait_send()
            else:
                link(array, pz, x, 1 - y, 2, x_mate).wait_send()

            @pl.when((z >= pz) & (z < Z_SIZE - 1))
            def _():
                link(array, pz, x, y, 0, up).wait_send()

            @pl.when((z <= pz) & (z > 0))
            def _():
                link(array, pz, x, y, 1, down).wait_send()


def gather_tiles(shards):
    any_space = pl.BlockSpec(memory_space=pl.ANY)
    count = len(shards)
    return pl.pallas_call(
        gather_kernel,
        out_shape=[jax.ShapeDtypeStruct((4, s.shape[0], 1024), s.dtype) for s in shards],
        in_specs=[any_space] * count,
        out_specs=[any_space] * count,
        scratch_shapes=[
            pltpu.SemaphoreType.DMA((count,)),
            pltpu.SemaphoreType.DMA((count, 16)),
            pltpu.SemaphoreType.DMA((count, 16)),
            pltpu.SemaphoreType.DMA((count, 5, 16)),
        ],
        compiler_params=pltpu.CompilerParams(
            collective_id=0, has_side_effects=True, vmem_limit_bytes=4 << 20
        ),
        name="gather_tiles",
    )(*shards)


def add_rows(target, terms, low):
    rows = 64

    def chunk(index, carry):
        at = pl.ds(pl.multiple_of(index * rows, rows), rows)
        total = terms[0][at, :].astype(jnp.float32)
        for term in terms[1:]:
            total = total + term[at, :].astype(jnp.float32)
        target[at, :] = total.astype(jnp.bfloat16) if low else total
        return carry

    lax.fori_loop(0, target.shape[0] // rows, chunk, 0)


def scatter_kernel(*refs):
    count = 4
    gain_ref, gain_out, gain_held, gain_in, gain_line, gain_send, gain_recv = (
        refs[count],
        refs[2 * count + 1],
        *refs[-5:],
    )
    refs = refs[:count] + refs[count + 1 : 2 * count + 1] + refs[2 * count + 2 : -5]
    wholes, outs = refs[:count], refs[count : 2 * count]
    held, twins, firsts, seconds, lines, totals = (
        refs[2 * count + count * k : 3 * count + count * k] for k in range(6)
    )
    load_sem, twin_send, twin_recv, link_send, link_recv, line_send, line_recv, out_sem = refs[
        8 * count :
    ]
    z, x, y, core = chip_coordinates()
    greet(z, x, y, core)
    x_mate, y_mate = device_of(z, 1 - x, y, core), device_of(z, x, 1 - y, core)
    up, down = device_of(z + 1, x, y, core), device_of(z - 1, x, y, core)

    def spot(array, pz, px, py, pcore):
        return wholes[array].at[py * 2 + pcore, :, pl.ds((pz * 2 + px) * 128, 128)]

    def chip_id(pz, px, py):
        return (pz * 2 + px) * 2 + py

    def load(array, pz, px, py):
        index = chip_id(pz, px, py)
        return pltpu.make_async_copy(
            spot(array, pz, px, py, core), held[array].at[index], load_sem.at[array, index]
        )

    def twin(array, pz, px, py):
        index = chip_id(pz, px, py)
        return pltpu.make_async_remote_copy(
            src_ref=spot(array, pz, px, py, 1 - core),
            dst_ref=twins[array].at[index],
            send_sem=twin_send.at[array, index],
            recv_sem=twin_recv.at[array, index],
            device_id=device_of(z, x, y, 1 - core),
            device_id_type=MESH_IDS,
        )

    def send(array, pz, px, py, inbox, slot, send_at, recv_at, target):
        return pltpu.make_async_remote_copy(
            src_ref=held[array].at[chip_id(pz, px, py)],
            dst_ref=inbox[array].at[slot],
            send_sem=send_at,
            recv_sem=recv_at,
            device_id=target,
            device_id_type=MESH_IDS,
        )

    def first(array, pz, same):
        if array in FIRST_X:
            px, py, target = (x if same else 1 - x), 1 - y, y_mate
        else:
            px, py, target = 1 - x, (y if same else 1 - y), x_mate
        slot = pz * 2 + same
        return (px, py), send(
            array,
            pz,
            px,
            py,
            firsts,
            slot,
            link_send.at[array, slot],
            link_recv.at[array, slot],
            target,
        )

    def second(array, pz):
        px, py, target = (1 - x, y, x_mate) if array in FIRST_X else (x, 1 - y, y_mate)
        return (px, py), send(
            array,
            pz,
            px,
            py,
            seconds,
            pz,
            link_send.at[array, 8 + pz],
            link_recv.at[array, 8 + pz],
            target,
        )

    def line(array, pz, upward, slot):
        return send(
            array,
            pz,
            x,
            y,
            lines,
            slot,
            line_send.at[array, pz],
            line_recv.at[array, slot],
            up if upward else down,
        )

    gain_mates = (device_of(z, x, y, 1 - core), x_mate, y_mate)

    def gain_copy(step):
        return pltpu.make_async_remote_copy(
            src_ref=gain_held.at[step],
            dst_ref=gain_in.at[step],
            send_sem=gain_send.at[step],
            recv_sem=gain_recv.at[step],
            device_id=gain_mates[step],
            device_id_type=MESH_IDS,
        )

    def gain_across(step):
        return pltpu.make_async_remote_copy(
            src_ref=gain_held.at[3],
            dst_ref=gain_line.at[step - 1],
            send_sem=gain_send.at[2 + step],
            recv_sem=gain_recv.at[2 + step],
            device_id=device_of((z + step) % Z_SIZE, x, y, core),
            device_id_type=MESH_IDS,
        )

    def gain_add(step):
        gain_copy(step).wait_recv()
        gain_held[step + 1] = gain_held[step] + gain_in[step]
        if step < 2:
            gain_copy(step + 1).start()
        else:
            for away in range(1, Z_SIZE):
                gain_across(away).start()

    def gain_finish():
        for away in range(1, Z_SIZE):
            gain_across(away).wait_recv()
        total = None
        for pz in range(Z_SIZE):
            term = jnp.where(z == pz, gain_held[3], 0.0)
            for away in range(1, Z_SIZE):
                sender = (z + Z_SIZE - away) % Z_SIZE
                term = jnp.where(sender == pz, gain_line[away - 1], term)
            total = term if total is None else total + term
        gain_out[...] = total
        for step in range(3):
            gain_copy(step).wait_send()
        for away in range(1, Z_SIZE):
            gain_across(away).wait_send()

    gain_held[0] = gain_ref[...]
    gain_copy(0).start()
    order = (1, 3, 2, 0)

    def begin(array, pz, px, py):
        load(array, pz, px, py).start()
        twin(array, pz, px, py).start()

    spread = (0, 3, 1, 2)
    for same in (0, 1):
        for pz in spread:
            for array in order:
                px, py = (
                    ((x if same else 1 - x), 1 - y)
                    if array in FIRST_X
                    else (1 - x, (y if same else 1 - y))
                )
                begin(array, pz, px, py)
    for pz in spread:
        for array in order:
            px, py = (1 - x, y) if array in FIRST_X else (x, 1 - y)
            begin(array, pz, px, py)
    for pz in spread:
        for array in order:
            begin(array, pz, x, y)

    def arrive(array, pz, px, py):
        load(array, pz, px, py).wait()
        twin(array, pz, px, py).wait_recv()
        index = chip_id(pz, px, py)
        return held[array].at[index], twins[array].at[index]

    for same in (0, 1):
        for pz in spread:
            for array in order:
                (px, py), moved = first(array, pz, same)
                mine, other = arrive(array, pz, px, py)
                add_rows(mine, (mine, other), True)
                moved.start()
        gain_add(same)
    for pz in spread:
        for array in order:
            (px, py), moved = second(array, pz)
            mine, other = arrive(array, pz, px, py)
            first(array, pz, 0)[1].wait_recv()
            add_rows(mine, (mine, other, firsts[array].at[pz * 2]), True)
            moved.start()

    gain_add(2)

    def terms_of(array, pz):
        mine, other = arrive(array, pz, x, y)
        first(array, pz, 1)[1].wait_recv()
        second(array, pz)[1].wait_recv()
        return mine, (mine, other, firsts[array].at[pz * 2 + 1], seconds[array].at[pz])

    for step in range(Z_SIZE - 1, 0, -1):
        for array in order:

            @pl.when(z + step <= Z_SIZE - 1)
            def _():
                pz = z + step
                mine, terms = terms_of(array, pz)
                moved = line(array, pz, True, step - 1)

                @pl.when(z == 0)
                def _():
                    add_rows(mine, terms, True)

                @pl.when(z > 0)
                def _():
                    line(array, pz, True, step).wait_recv()
                    add_rows(mine, terms + (lines[array].at[step],), True)

                moved.start()

            @pl.when(z >= step)
            def _():
                pz = z - step
                mine, terms = terms_of(array, pz)
                moved = line(array, pz, False, Z_SIZE + step - 1)

                @pl.when(z == Z_SIZE - 1)
                def _():
                    add_rows(mine, terms, True)

                @pl.when(z < Z_SIZE - 1)
                def _():
                    line(array, pz, False, Z_SIZE + step).wait_recv()
                    add_rows(mine, terms + (lines[array].at[Z_SIZE + step],), True)

                moved.start()

    for array in order:
        mine, terms = terms_of(array, z)
        from_below, from_above = lines[array].at[0], lines[array].at[Z_SIZE]

        @pl.when(z == 0)
        def _():
            line(array, z, False, Z_SIZE).wait_recv()
            add_rows(totals[array], terms + (from_above,), False)

        @pl.when(z == Z_SIZE - 1)
        def _():
            line(array, z, True, 0).wait_recv()
            add_rows(totals[array], terms + (from_below,), False)

        @pl.when((z > 0) & (z < Z_SIZE - 1))
        def _():
            line(array, z, True, 0).wait_recv()
            line(array, z, False, Z_SIZE).wait_recv()
            add_rows(totals[array], terms + (from_below, from_above), False)

        pltpu.make_async_copy(totals[array], outs[array], out_sem.at[array]).start()

    gain_finish()
    for array in order:
        pltpu.make_async_copy(totals[array], outs[array], out_sem.at[array]).wait()
        for pz in range(Z_SIZE):
            for px in range(2):
                for py in range(2):
                    twin(array, pz, px, py).wait_send()
            first(array, pz, 0)[1].wait_send()
            first(array, pz, 1)[1].wait_send()
            second(array, pz)[1].wait_send()

            @pl.when(z != pz)
            def _():
                line(array, pz, True, 0).wait_send()


def scatter_tiles(wholes, gains):
    any_space = pl.BlockSpec(memory_space=pl.ANY)
    count = len(wholes)
    sizes = [w.shape[1] for w in wholes]

    def boxes(slots, kind=jnp.bfloat16):
        return [pltpu.VMEM((slots, n, 128), kind) for n in sizes]

    return pl.pallas_call(
        scatter_kernel,
        out_shape=[jax.ShapeDtypeStruct((n, 128), jnp.float32) for n in sizes]
        + [jax.ShapeDtypeStruct(gains.shape, jnp.float32)],
        in_specs=[any_space] * count + [pl.BlockSpec(memory_space=pltpu.VMEM)],
        out_specs=[any_space] * count + [pl.BlockSpec(memory_space=pltpu.VMEM)],
        scratch_shapes=boxes(16)
        + boxes(16)
        + boxes(8)
        + boxes(4)
        + boxes(8)
        + [pltpu.VMEM((n, 128), jnp.float32) for n in sizes]
        + [
            pltpu.SemaphoreType.DMA((count, 16)),
            pltpu.SemaphoreType.DMA((count, 16)),
            pltpu.SemaphoreType.DMA((count, 16)),
            pltpu.SemaphoreType.DMA((count, 12)),
            pltpu.SemaphoreType.DMA((count, 12)),
            pltpu.SemaphoreType.DMA((count, 4)),
            pltpu.SemaphoreType.DMA((count, 8)),
            pltpu.SemaphoreType.DMA((count,)),
            pltpu.VMEM((4,) + gains.shape, jnp.float32),
            pltpu.VMEM((3,) + gains.shape, jnp.float32),
            pltpu.VMEM((3,) + gains.shape, jnp.float32),
            pltpu.SemaphoreType.DMA((6,)),
            pltpu.SemaphoreType.DMA((6,)),
        ],
        compiler_params=pltpu.CompilerParams(
            collective_id=1, has_side_effects=True, vmem_limit_bytes=56 << 20
        ),
        name="scatter_tiles",
    )(*wholes, gains)


def slot_body(
    hidden_in,
    first_values,
    lengths,
    places,
    gain_attn,
    gain_ffn,
    w_query,
    w_key,
    w_value,
    w_out,
    w_gate,
    w_up,
    w_down,
    out_grad,
):
    slots, rows, width = hidden_in.shape
    count = slots * rows
    heads = width // HEAD_DIM
    hidden_tile = w_gate.shape[1]
    column = lax.axis_index("col")
    score_scale = HEAD_DIM ** (-0.5)
    ff = hidden_tile * slots
    wide = w_query.shape[1]
    near = jnp.concatenate([w_query.T, w_key.T, w_value.T, w_out], axis=0)
    near_all, gate_all, up_all, down_all = gather_tiles((near, w_gate.T, w_up.T, w_down))
    wq, wk, wv, wo = (
        near_all[:, k * wide : (k + 1) * wide].reshape(width, width) for k in range(4)
    )
    wg, wu, wd = (whole.reshape(ff, width) for whole in (gate_all, up_all, down_all))

    first_rows = jnp.transpose(first_values, (0, 2, 1))
    feature_tile = first_rows.shape[2]
    first_packed = first_rows.reshape(slots, slots, rows, feature_tile)
    first_packed = jnp.transpose(first_packed, (0, 2, 1, 3)).reshape(slots, rows, width)
    sent = jnp.concatenate([hidden_in, out_grad, first_packed], axis=1)
    got = lax.all_to_all(sent, "col", split_axis=0, concat_axis=0, tiled=True)
    hidden = got[:, :rows].reshape(count, width).astype(jnp.float32)
    grad_rows = got[:, rows : 2 * rows].reshape(count, width)
    first = got[:, 2 * rows :].reshape(slots, rows, slots, feature_tile)
    first = jnp.transpose(first, (2, 1, 0, 3)).reshape(count, width).astype(jnp.float32)

    place = lax.dynamic_index_in_dim(places, column, 0, keepdims=False)
    length = lax.dynamic_index_in_dim(lengths, column, 0, keepdims=False)
    ends_at = jnp.cumsum(length)
    starts_at = ends_at - length
    past = place[:, None] >= ends_at[None, :]
    segment_id = jnp.sum(past.astype(jnp.int32), axis=1)
    one_hot = segment_id[:, None] == jnp.arange(length.shape[0], dtype=jnp.int32)[None, :]
    position = place - jnp.sum(jnp.where(one_hot, starts_at[None, :], 0), axis=1)
    cosine, sine = rotary_tables(position)
    allowed = (segment_id[:, None] == segment_id[None, :]) & (place[:, None] >= place[None, :])

    scale_one = lax.rsqrt(jnp.mean(hidden * hidden, axis=1, keepdims=True) + EPSILON)
    normed_one = (hidden * scale_one * gain_attn).astype(jnp.bfloat16)
    by_head = (count, heads, HEAD_DIM)
    queries = rotate(product_right(normed_one, wq).reshape(by_head), cosine, sine).astype(jnp.bfloat16)
    keys = rotate(product_right(normed_one, wk).reshape(by_head), cosine, sine).astype(jnp.bfloat16)
    values = (0.5 * product_right(normed_one, wv) + 0.5 * first).astype(jnp.bfloat16).reshape(by_head)

    raw_scores = jnp.einsum("qhd,khd->hqk", queries, keys, preferred_element_type=jnp.float32)
    scores = jnp.where(allowed[None], raw_scores * score_scale, MASKED)
    row_top = jnp.max(scores, axis=-1, keepdims=True)
    log_total = row_top + jnp.log(jnp.sum(jnp.exp(scores - row_top), axis=-1, keepdims=True))
    probs = jnp.exp(scores - log_total)
    probs_low = probs.astype(jnp.bfloat16)
    attended = (
        jnp.einsum("hqk,khd->qhd", probs_low, values, preferred_element_type=jnp.float32)
        .astype(jnp.bfloat16)
        .reshape(count, width)
    )
    mid = hidden + product(attended, wo)
    scale_two = lax.rsqrt(jnp.mean(mid * mid, axis=1, keepdims=True) + EPSILON)
    normed_two = (mid * scale_two * gain_ffn).astype(jnp.bfloat16)
    gate_raw = product_right(normed_two, wg)
    up_raw = product_right(normed_two, wu)
    sigmoid_gate = jax.nn.sigmoid(gate_raw)
    silu_gate = gate_raw * sigmoid_gate
    hidden_act = (silu_gate * up_raw).astype(jnp.bfloat16)
    stored_out = (mid + product(hidden_act, wd)).astype(jnp.bfloat16)

    def pieces(left, right):
        grad = product_left(left, right).astype(jnp.bfloat16)
        return grad.reshape(slots, grad.shape[0] // slots, width)

    grad_down = pieces(hidden_act, grad_rows)
    d_hidden = product_right(grad_rows, wd)
    d_gate = (d_hidden * up_raw * sigmoid_gate * (1.0 + gate_raw * (1.0 - sigmoid_gate))).astype(
        jnp.bfloat16
    )
    d_up = (d_hidden * silu_gate).astype(jnp.bfloat16)
    grad_gate = pieces(d_gate, normed_two)
    grad_up = pieces(d_up, normed_two)
    d_normed_two = product(d_gate, wg) + product(d_up, wu)
    gain_sum_two = jnp.sum(d_normed_two * mid * scale_two, axis=0)
    scaled_two = d_normed_two * gain_ffn
    stat_two = jnp.sum(scaled_two * mid, axis=1, keepdims=True)
    d_mid = (
        grad_rows.astype(jnp.float32)
        + scale_two * scaled_two
        - mid * (scale_two * scale_two * scale_two * stat_two / width)
    )
    d_branch = d_mid.astype(jnp.bfloat16)
    grad_out = pieces(attended, d_branch)
    d_attended = product_right(d_branch, wo).astype(jnp.bfloat16).reshape(by_head)
    d_probs = jnp.einsum("qhd,khd->hqk", d_attended, values, preferred_element_type=jnp.float32)
    inner_sum = jnp.sum(probs * d_probs, axis=-1, keepdims=True)
    d_scores = (probs * (d_probs - inner_sum)).astype(jnp.bfloat16)
    d_query = score_scale * jnp.einsum(
        "hqk,khd->qhd", d_scores, keys, preferred_element_type=jnp.float32
    )
    d_key = score_scale * jnp.einsum(
        "hqk,qhd->khd", d_scores, queries, preferred_element_type=jnp.float32
    )
    d_values = (
        jnp.einsum("hqk,qhd->khd", probs_low, d_attended, preferred_element_type=jnp.float32)
        .astype(jnp.bfloat16)
        .reshape(count, width)
    )
    d_value_proj = (0.5 * d_values.astype(jnp.float32)).astype(jnp.bfloat16)
    d_query_raw = rotate_back(d_query, cosine, sine).astype(jnp.bfloat16).reshape(count, width)
    d_key_raw = rotate_back(d_key, cosine, sine).astype(jnp.bfloat16).reshape(count, width)
    grad_query = pieces(d_query_raw, normed_one)
    grad_key = pieces(d_key_raw, normed_one)
    grad_value = pieces(d_value_proj, normed_one)
    d_normed_one = (
        product(d_query_raw, wq)
        + product(d_key_raw, wk)
        + product(d_value_proj, wv)
    )
    gain_sum_one = jnp.sum(d_normed_one * hidden * scale_one, axis=0)
    scaled_one = d_normed_one * gain_attn
    stat_one = jnp.sum(scaled_one * hidden, axis=1, keepdims=True)
    input_grad = (
        d_mid
        + scale_one * scaled_one
        - hidden * (scale_one * scale_one * scale_one * stat_one / width)
    )
    value_sent = d_value_proj.reshape(slots, rows, slots, feature_tile)
    value_sent = jnp.transpose(value_sent, (2, 1, 0, 3)).reshape(slots, rows, width)
    sent_back = jnp.concatenate(
        [
            stored_out.reshape(slots, rows, width),
            input_grad.astype(jnp.bfloat16).reshape(slots, rows, width),
            value_sent,
        ],
        axis=1,
    )
    back = lax.all_to_all(sent_back, "col", split_axis=0, concat_axis=0, tiled=True)
    value_back = back[:, 2 * rows :].reshape(slots, rows, slots, feature_tile)
    value_back = jnp.transpose(value_back, (0, 3, 2, 1)).reshape(slots, feature_tile, count)
    grad_near = jnp.concatenate([grad_query, grad_key, grad_value, grad_out], axis=1)
    gains = jnp.concatenate([gain_sum_one, gain_sum_two]).reshape(-1, 128)
    near_tile, gate_tile, up_tile, down_tile, gain_total = scatter_tiles(
        (grad_near, grad_gate, grad_up, grad_down), gains
    )
    gain_total = gain_total.reshape(2, width)
    return (
        back[:, :rows],
        back[:, rows : 2 * rows].astype(jnp.float32),
        value_back.astype(jnp.float32),
        gain_total[0],
        gain_total[1],
        near_tile[:wide].T,
        near_tile[wide : 2 * wide].T,
        near_tile[2 * wide : 3 * wide].T,
        near_tile[3 * wide :],
        gate_tile.T,
        up_tile.T,
        down_tile,
    )


def solution(mesh):
    def body(*arrays):
        one_each = mesh.shape["row"] == 2 * Z_SIZE and arrays[0].shape[0] == mesh.shape["col"] == 4
        return (slot_body if one_each else tiled_body)(*arrays)

    return jax.shard_map(
        body,
        mesh=mesh,
        in_specs=(
            P("row", "col", None),
            P("row", "col", None),
            P("row", None),
            P("row", None),
            P(),
            P(),
            P("row", "col"),
            P("row", "col"),
            P("row", "col"),
            P("col", "row"),
            P("row", "col"),
            P("row", "col"),
            P("col", "row"),
            P("row", "col", None),
        ),
        out_specs=(
            P("row", "col", None),
            P("row", "col", None),
            P("row", "col", None),
            P(),
            P(),
            P("row", "col"),
            P("row", "col"),
            P("row", "col"),
            P("col", "row"),
            P("row", "col"),
            P("row", "col"),
            P("col", "row"),
        ),
        check_vma=False,
    )
```
